32 devices in a mesh: dp: 2 (over z, core), tp: 16 (over x, y).
Axes of the slice: x: 4, y: 4, z: 1, core: 2. Of those that a mesh axis runs over, the one named last changes fastest.
The devices are a block of a 4x4x8 slice.
Arguments:
- x: bfloat16 [256, 8192], P('dp'), parts along dimension 0
- w_gate: bfloat16 [8192, 24576], P(None, 'tp')
- w_up: bfloat16 [8192, 24576], P(None, 'tp')
- w_down: bfloat16 [24576, 8192], P('tp')
Outputs:
- output: bfloat16 [256, 8192], P('dp'), parts along dimension 0
There are 2 independent parts. The reference program is written for one: setup_inputs(seed, part) draws one part's arguments, and reference() takes and returns one part's arrays. A program takes and returns all parts, laid end to end along the dimension named above; an argument that names none is the same for every part.
All inputs are finite; a program needn't handle non-finite values.
Results may differ from the reference program's by a relative error of at most 0.016.
Values are sent between devices in bfloat16 or wider.
A program may use at most 768 MiB of HBM per device.

```python
import jax
import jax.numpy as jnp

ROWS = 128
D = 8192
FF = 24576


def setup_inputs(seed: int = 0, part: int = 0) -> dict:
    kx, kg, ku, kd = jax.random.split(jax.random.key(seed), 4)
    drawn = {
        "x": jax.random.normal(jax.random.fold_in(kx, part), (ROWS, D), jnp.float32),
        "w_gate": jax.random.normal(kg, (D, FF), jnp.float32) * D**-0.5,
        "w_up": jax.random.normal(ku, (D, FF), jnp.float32) * D**-0.5,
        "w_down": jax.random.normal(kd, (FF, D), jnp.float32) * FF**-0.5,
    }
    return {k: v.astype(jnp.bfloat16) for k, v in drawn.items()}


def reference(x, w_gate, w_up, w_down):
    gate = jnp.dot(x, w_gate, preferred_element_type=jnp.float32)
    up = jnp.dot(x, w_up, preferred_element_type=jnp.float32)
    hidden = (jax.nn.silu(gate) * up).astype(jnp.bfloat16)
    return jnp.dot(hidden, w_down, preferred_element_type=jnp.float32).astype(jnp.bfloat16)
```

```python
import functools

import jax
import jax.numpy as jnp
from jax import lax
from jax.experimental import pallas as pl
from jax.experimental.pallas import tpu as pltpu
from jax.sharding import PartitionSpec as P

MESH = pl.DeviceIdType.MESH
CHUNKS = 2
NBLOCK = 512
KCHUNK = 1024
DEPTH = 4
AHEAD = 4
BF16, F32 = jnp.bfloat16, jnp.float32


def kernel(
    chunks, kchunk, nblock, depth,
    x_hbm, wg_hbm, wu_hbm, wd_hbm, y,
    xv, gb, ub, wdb, accg, accu, hid,
    own, keep, sstep, sdir, smrg, rstep, rdir, rmrg,
    tstep, tdir, tmrg, qstep, qdir, qmrg,
    xsem, gsem, usem, wsem, ssem, rsem,
):
    n = lax.axis_size("tp")
    side = 4
    me = lax.axis_index("tp")
    px, py = me // side, lax.rem(me, side)

    def at(i, j):
        return lax.rem(i + side, side) * side + lax.rem(j + side, side)

    axes = (
        ((px, at(px + 1, py), at(px - 1, py)), (py, at(px, py + 1), at(px, py - 1))),
        ((py, at(px, py + 1), at(px, py - 1)), (px, at(px + 1, py), at(px - 1, py))),
    )

    barrier = pltpu.get_barrier_semaphore()
    for _, plus, minus in axes[0]:
        for dev in (plus, minus):
            pl.semaphore_signal(barrier, inc=1, device_id={"tp": dev}, device_id_type=MESH)

    rows = xv.shape[1]
    ksteps = wg_hbm.shape[0] // kchunk
    nblocks = wg_hbm.shape[1] // nblock
    steps = ksteps * nblocks
    width = y.shape[1] // (2 * chunks * side)
    half, quarter, eighth = rows // 2, rows // 4, rows // 8

    def xcopy(k):
        return pltpu.make_async_copy(x_hbm.at[:, pl.ds(k * kchunk, kchunk)], xv.at[k], xsem.at[k])

    def gcopy(i, slot):
        nb, k = i // ksteps, lax.rem(i, ksteps)
        src = (pl.ds(k * kchunk, kchunk), pl.ds(nb * nblock, nblock))
        return (
            pltpu.make_async_copy(wg_hbm.at[src], gb.at[slot], gsem.at[slot]),
            pltpu.make_async_copy(wu_hbm.at[src], ub.at[slot], usem.at[slot]),
        )

    def cols(h, c, seg):
        return pl.ds(pl.multiple_of(((h * chunks + c) * side + seg) * width, width), width)

    order = []
    for c in range(chunks):
        for off in (2, 1, 3, 0):
            for h in range(2):
                order.append((h, c, off))

    def wcopy(j):
        h, c, off = order[j]
        seg = lax.rem(axes[h][0][0] + off, side)
        return pltpu.make_async_copy(wd_hbm.at[:, cols(h, c, seg)], wdb.at[j], wsem.at[j])

    for i in range(depth):
        xcopy(i).start()
        for cp in gcopy(jnp.int32(i), i):
            cp.start()
    for k in range(depth, ksteps):
        xcopy(k).start()

    for nb in range(nblocks):
        accg[...] = jnp.zeros_like(accg)
        accu[...] = jnp.zeros_like(accu)

        @pl.loop(0, ksteps)
        def _(k, nb=nb):
            i = nb * ksteps + k
            slot = lax.rem(i, depth)
            if nb == 0:
                xcopy(k).wait()
            for cp in gcopy(i, slot):
                cp.wait()
            accg[...] += jnp.dot(xv[k], gb[slot], preferred_element_type=F32)
            accu[...] += jnp.dot(xv[k], ub[slot], preferred_element_type=F32)

            @pl.when(i + depth < steps)
            def _():
                for cp in gcopy(i + depth, slot):
                    cp.start()

            if nb == nblocks - 1:
                for d in range(depth):

                    @pl.when(i + depth == steps + d)
                    def _(d=d):
                        if d < len(order):
                            wcopy(d).start()

        g = accg[...]
        hid[:, nb * nblock : (nb + 1) * nblock] = (jax.nn.silu(g) * accu[...]).astype(BF16)

    copies = {}

    def send(h, c, key, slot, src, dst, dev):
        cp = pltpu.make_async_remote_copy(
            src_ref=src, dst_ref=dst, send_sem=ssem.at[h, c, slot], recv_sem=rsem.at[h, c, slot],
            device_id={"tp": dev}, device_id_type=MESH,
        )
        cp.start()
        copies[h, c, key] = cp

    def term(j):
        if j + depth < len(order):
            wcopy(j + depth).start()
        wcopy(j).wait()
        return jnp.dot(hid[...], wdb[j], preferred_element_type=F32)

    def compute(j):
        h, c, off = order[j]
        _, plus, minus = axes[h][0]
        t = term(j)
        if off == 2:
            sstep[h, c] = t.astype(BF16)
            send(h, c, "step+", 0, sstep.at[h, c, :half], rstep.at[h, c, 0], plus)
            send(h, c, "step-", 1, sstep.at[h, c, half:], rstep.at[h, c, 1], minus)
        elif off == 1:
            keep[h, c, 0] = t[:half]
            sdir[h, c, 0] = t[half:].astype(BF16)
            send(h, c, "dir+", 2, sdir.at[h, c, 0], rdir.at[h, c, 0], plus)
        elif off == 3:
            keep[h, c, 1] = t[half:]
            sdir[h, c, 1] = t[:half].astype(BF16)
            send(h, c, "dir-", 3, sdir.at[h, c, 1], rdir.at[h, c, 1], minus)
        else:
            own[h, c] = t

    def merge(h, c):
        _, plus, minus = axes[h][0]
        for d, dev in enumerate((plus, minus)):
            copies[h, c, "step" + "+-"[d]].wait_recv()
            smrg[h, c, d] = (keep[h, c, d] + rstep[h, c, d].astype(F32)).astype(BF16)
            send(h, c, "mrg" + "+-"[d], 4 + d, smrg.at[h, c, d], rmrg.at[h, c, d], dev)

    def sub(p, off, first=0):
        return pl.multiple_of(lax.rem(p + off, side) * quarter + first, eighth)

    def second(h, c):
        for key in ("dir+", "dir-", "mrg+", "mrg-"):
            copies[h, c, key].wait_recv()
        own[h, c, :half] = own[h, c, :half] + (rmrg[h, c, 0].astype(F32) + rdir[h, c, 1].astype(F32))
        own[h, c, half:] = own[h, c, half:] + (rmrg[h, c, 1].astype(F32) + rdir[h, c, 0].astype(F32))
        p, plus, minus = axes[h][1]
        tstep[h, c] = own[h, c, pl.ds(sub(p, 2), quarter)].astype(BF16)
        tdir[h, c, 0] = own[h, c, pl.ds(sub(p, 1, eighth), eighth)].astype(BF16)
        tdir[h, c, 1] = own[h, c, pl.ds(sub(p, 3), eighth)].astype(BF16)
        send(h, c, "step2+", 6, tstep.at[h, c, :eighth], qstep.at[h, c, 0], plus)
        send(h, c, "step2-", 7, tstep.at[h, c, eighth:], qstep.at[h, c, 1], minus)
        send(h, c, "dir2+", 8, tdir.at[h, c, 0], qdir.at[h, c, 0], plus)
        send(h, c, "dir2-", 9, tdir.at[h, c, 1], qdir.at[h, c, 1], minus)

    def merge2(h, c):
        p, plus, minus = axes[h][1]
        for d, dev in enumerate((plus, minus)):
            copies[h, c, "step2" + "+-"[d]].wait_recv()
            mine = own[h, c, pl.ds(sub(p, 1 + 2 * d, eighth * d), eighth)]
            tmrg[h, c, d] = (mine + qstep[h, c, d].astype(F32)).astype(BF16)
            send(h, c, "mrg2" + "+-"[d], 10 + d, tmrg.at[h, c, d], qmrg.at[h, c, d], dev)

    def gather(h, c):
        for key in ("dir2+", "dir2-", "mrg2+", "mrg2-"):
            copies[h, c, key].wait_recv()
        p, plus, minus = axes[h][1]
        pf = axes[h][0][0]
        top = own[h, c, pl.ds(sub(p, 0), eighth)]
        low = own[h, c, pl.ds(sub(p, 0, eighth), eighth)]
        top += qmrg[h, c, 0].astype(F32) + qdir[h, c, 1].astype(F32)
        low += qmrg[h, c, 1].astype(F32) + qdir[h, c, 0].astype(F32)
        y[pl.ds(sub(p, 0), eighth), cols(h, c, pf)] = top.astype(BF16)
        y[pl.ds(sub(p, 0, eighth), eighth), cols(h, c, pf)] = low.astype(BF16)
        mine = y.at[pl.ds(sub(p, 0), quarter), cols(h, c, pf)]
        send(h, c, "ag+", 12, mine, mine, plus)
        send(h, c, "ag-", 13, mine, mine, minus)

    def relay(h, c):
        p, plus, minus = axes[h][1]
        pf = axes[h][0][0]
        for d, dev in enumerate((plus, minus)):
            copies[h, c, "ag" + "+-"[d]].wait_recv()
            piece = y.at[pl.ds(sub(p, 3 - 2 * d, eighth * d), eighth), cols(h, c, pf)]
            send(h, c, "rl" + "+-"[d], 14 + d, piece, piece, dev)

    def gather2(h, c):
        copies[h, c, "rl+"].wait_recv()
        copies[h, c, "rl-"].wait_recv()
        pf, plus, minus = axes[h][0]
        mine = y.at[:, cols(h, c, pf)]
        send(h, c, "ag2+", 16, mine, mine, plus)
        send(h, c, "ag2-", 17, mine, mine, minus)

    def relay2(h, c):
        pf, plus, minus = axes[h][0]
        for d, dev in enumerate((plus, minus)):
            copies[h, c, "ag2" + "+-"[d]].wait_recv()
            seg = lax.rem(pf + 3 - 2 * d, side)
            piece = y.at[pl.ds(half * d, half), cols(h, c, seg)]
            send(h, c, "rl2" + "+-"[d], 18 + d, piece, piece, dev)

    def last(h, c):
        copies[h, c, "rl2+"].wait_recv()
        copies[h, c, "rl2-"].wait_recv()

    pl.semaphore_wait(barrier, 4)

    stages = (merge, second, merge2, gather, relay, gather2, relay2, last)
    for tick in range(chunks + len(stages)):
        if tick < chunks:
            for j in range(8 * tick, 8 * tick + 8):
                compute(j)
        for s in reversed(range(len(stages))):
            c = tick - s
            if 0 <= c < chunks:
                for h in range(2):
                    stages[s](h, c)

    for cp in copies.values():
        cp.wait_send()


def block(n, x, w_gate, w_up, w_down):
    rows, d = x.shape
    ff = w_gate.shape[1]
    side = 4
    assert n == side * side
    c = CHUNKS
    width = d // (2 * c * side)
    kchunk, nblock = min(KCHUNK, d), min(NBLOCK, ff)
    half, eighth = rows // 2, rows // 8
    vm = pltpu.VMEM
    dma = pltpu.SemaphoreType.DMA
    hbm = pl.BlockSpec(memory_space=pltpu.HBM)
    return pl.pallas_call(
        functools.partial(kernel, c, kchunk, nblock, DEPTH),
        out_shape=jax.ShapeDtypeStruct((rows, d), BF16),
        in_specs=[hbm] * 4,
        out_specs=pl.BlockSpec(memory_space=pltpu.VMEM),
        scratch_shapes=[
            vm((d // kchunk, rows, kchunk), BF16),
            vm((DEPTH, kchunk, nblock), BF16),
            vm((DEPTH, kchunk, nblock), BF16),
            vm((2 * c * side, ff, width), BF16),
            vm((rows, nblock), F32),
            vm((rows, nblock), F32),
            vm((rows, ff), BF16),
            vm((2, c, rows, width), F32),
            vm((2, c, 2, half, width), F32),
            vm((2, c, rows, width), BF16),
            vm((2, c, 2, half, width), BF16),
            vm((2, c, 2, half, width), BF16),
            vm((2, c, 2, half, width), BF16),
            vm((2, c, 2, half, width), BF16),
            vm((2, c, 2, half, width), BF16),
            vm((2, c, 2 * eighth, width), BF16),
            vm((2, c, 2, eighth, width), BF16),
            vm((2, c, 2, eighth, width), BF16),
            vm((2, c, 2, eighth, width), BF16),
            vm((2, c, 2, eighth, width), BF16),
            vm((2, c, 2, eighth, width), BF16),
            dma((d // kchunk,)),
            dma((DEPTH,)),
            dma((DEPTH,)),
            dma((2 * c * side,)),
            dma((2, c, 20)),
            dma((2, c, 20)),
        ],
        compiler_params=pltpu.CompilerParams(
            collective_id=0, has_side_effects=True, vmem_limit_bytes=48 * 2**20
        ),
        name="mlp",
    )(x, w_gate, w_up, w_down)


def solution(mesh):
    return jax.shard_map(
        functools.partial(block, mesh.shape["tp"]),
        mesh=mesh,
        in_specs=(P("dp", None), P(None, "tp"), P(None, "tp"), P("tp", None)),
        out_specs=P("dp", None),
        check_vma=False,
    )
```

```python
import functools

import jax
import jax.numpy as jnp
from jax import lax
from jax.experimental import pallas as pl
from jax.experimental.pallas import tpu as pltpu
from jax.sharding import PartitionSpec as P

MESH = pl.DeviceIdType.MESH
BF16, F32 = jnp.bfloat16, jnp.float32
GROUPS = ((2,), (2,), (2,), (2,))
NBLOCK = 512
KCHUNK = 1024
DEPTH = 4
AHEAD = 5
SCHEDULE = ("X0", "X1", "X2", "X3", "Y0", "M0", "Y1", "M1", "Y2", "M2", "Y3", "M3", "S0", "S1", "S2", "S3", "G0", "G1", "G2", "G3", "A0", "A1", "D2", "D3", "R0", "R1", "L0", "L1", "E2", "E3")


def kernel(
    groups, kchunk, nblock,
    x_hbm, wg_hbm, wu_hbm, wd_hbm, y,
    xv, gub, wdb, accg, accu, hid,
    xsem, gusem, wsem, ssem, rsem, *chunk_refs,
):
    widths = [w for group in groups for w in group]
    split = 4 * len(groups)
    own, tsum, qsum, tmrg = (chunk_refs[i:split:4] for i in range(4))
    keep, sstep, sdir, smrg, rstep, rboth = (chunk_refs[split + i :: 6] for i in range(6))
    where = [(g, sum(group[:i])) for g, group in enumerate(groups) for i in range(len(group))]
    gwidths = [sum(group) for group in groups]

    side = 4
    me = lax.axis_index("tp")
    px, py = me // side, lax.rem(me, side)

    def at(i, j):
        return lax.rem(i + side, side) * side + lax.rem(j + side, side)

    along = (
        (px, at(px + 1, py), at(px - 1, py), at(px + 2, py)),
        (py, at(px, py + 1), at(px, py - 1), at(px, py + 2)),
    )
    axes = (along, along[::-1])

    rows = xv.shape[1]
    ksteps = wg_hbm.shape[0] // kchunk
    nblocks = wg_hbm.shape[1] // nblock
    steps = ksteps * nblocks
    half, quarter, eighth = rows // 2, rows // 4, rows // 8
    ring = wdb.shape[0]

    def xcopy(k):
        return pltpu.make_async_copy(x_hbm.at[:, pl.ds(k * kchunk, kchunk)], xv.at[k], xsem.at[k])

    def gstart(i, slot):
        nb, k = i // ksteps, lax.rem(i, ksteps)
        src = (pl.ds(k * kchunk, kchunk), pl.ds(nb * nblock, nblock))
        pltpu.make_async_copy(wg_hbm.at[src], gub.at[slot, 0], gusem.at[slot]).start()
        pltpu.make_async_copy(wu_hbm.at[src], gub.at[slot, 1], gusem.at[slot]).start()

    def gwait(slot):
        pltpu.make_async_copy(gub.at[slot], gub.at[slot], gusem.at[slot]).wait()

    def cols(h, g, seg, skip=0, width=None):
        first = h * sum(widths) * side + sum(gwidths[:g]) * side + skip
        return pl.ds(pl.multiple_of(first + seg * gwidths[g], 128), width or gwidths[g])

    plan = SCHEDULE
    order = []
    for token in plan:
        order += [(int(token[1]), off) for off in {"X": (2,), "Y": (1, 3, 0)}.get(token[0], ())]

    def wstart(j):
        c, off = order[j]
        g, skip = where[c]
        for h in range(2):
            seg = lax.rem(axes[h][0][0] + off, side)
            pltpu.make_async_copy(
                wd_hbm.at[:, cols(h, g, seg, skip, widths[c])],
                wdb.at[j % ring, :, h * widths[c] : (h + 1) * widths[c]],
                wsem.at[j % ring],
            ).start()

    def wwait(j):
        buf = wdb.at[j % ring, :, : 2 * widths[order[j][0]]]
        pltpu.make_async_copy(buf, buf, wsem.at[j % ring]).wait()

    for i in range(DEPTH):
        xcopy(i).start()
        gstart(jnp.int32(i), i)
    for k in range(DEPTH, ksteps):
        xcopy(k).start()

    barrier = pltpu.get_barrier_semaphore()
    for _, *partners in along:
        for dev in partners:
            pl.semaphore_signal(barrier, inc=1, device_id={"tp": dev}, device_id_type=MESH)

    for nb in range(nblocks):
        accg[...] = jnp.zeros_like(accg)
        accu[...] = jnp.zeros_like(accu)

        @pl.loop(0, ksteps)
        def _(k, nb=nb):
            i = nb * ksteps + k
            slot = lax.rem(i, DEPTH)
            if nb == 0:
                xcopy(k).wait()
            gwait(slot)
            accg[...] += jnp.dot(xv[k], gub[slot, 0], preferred_element_type=F32)
            accu[...] += jnp.dot(xv[k], gub[slot, 1], preferred_element_type=F32)

            @pl.when(i + DEPTH < steps)
            def _():
                gstart(i + DEPTH, slot)

            if nb == nblocks - 1:
                for d in range(DEPTH):

                    @pl.when(i + DEPTH == steps + d)
                    def _(d=d):
                        for j in range(d * AHEAD // DEPTH, (d + 1) * AHEAD // DEPTH):
                            wstart(j)

        g = accg[...]
        hid[:, nb * nblock : (nb + 1) * nblock] = (jax.nn.silu(g) * accu[...]).astype(BF16)

    sent = []

    def send(sem, src, dst, dev):
        pltpu.make_async_remote_copy(
            src_ref=src, dst_ref=dst, send_sem=ssem, recv_sem=rsem.at[sem],
            device_id={"tp": dev}, device_id_type=MESH,
        ).start()
        sent.append(src.shape[0] * src.shape[1])

    def arrived(sem, like):
        pltpu.make_async_copy(like, like, rsem.at[sem]).wait()

    def gsem(g, stage):
        return 2 * len(widths) + 6 * g + stage

    def down(offs, c):
        for off in offs:
            j = order.index((c, off))
            if j + AHEAD < len(order):
                wstart(j + AHEAD)
            wwait(j)
            width = widths[c]
            g, skip = where[c]
            both = jnp.dot(hid[...], wdb[j % ring, :, : 2 * width], preferred_element_type=F32)
            for h in range(2):
                _, plus, minus, _ = axes[h][0]
                t = both[:, h * width : (h + 1) * width]
                if off == 2:
                    sstep[c][h] = t.astype(BF16)
                    send(2 * c, sstep[c].at[h, :half], rstep[c].at[h, 0], plus)
                    send(2 * c, sstep[c].at[h, half:], rstep[c].at[h, 1], minus)
                elif off == 1:
                    keep[c][h, 0] = t[:half]
                    sdir[c][h, 0] = t[half:].astype(BF16)
                    send(2 * c + 1, sdir[c].at[h, 0], rboth[c].at[h, 2], plus)
                elif off == 3:
                    keep[c][h, 1] = t[half:]
                    sdir[c][h, 1] = t[:half].astype(BF16)
                    send(2 * c + 1, sdir[c].at[h, 1], rboth[c].at[h, 3], minus)
                else:
                    own[g][h, :, skip : skip + width] = t

    def merge(c):
        arrived(2 * c, rstep[c])
        for h in range(2):
            _, plus, minus, _ = axes[h][0]
            for d, dev in enumerate((plus, minus)):
                smrg[c][h, d] = (keep[c][h, d] + rstep[c][h, d].astype(F32)).astype(BF16)
                send(2 * c + 1, smrg[c].at[h, d], rboth[c].at[h, d], dev)

    def sub(p, off):
        return pl.ds(pl.multiple_of(lax.rem(p + off, side) * quarter, quarter), quarter)

    def sub8(p, off, low):
        return pl.ds(pl.multiple_of(lax.rem(p + off, side) * quarter + low * eighth, eighth), eighth)

    def second(g):
        for c, (at_g, skip) in enumerate(where):
            if at_g != g:
                continue
            arrived(2 * c + 1, rboth[c])
            part = slice(skip, skip + widths[c])
            for h in range(2):
                top = own[g][h, :half, part] + (rboth[c][h, 0].astype(F32) + rboth[c][h, 3].astype(F32))
                low = own[g][h, half:, part] + (rboth[c][h, 1].astype(F32) + rboth[c][h, 2].astype(F32))
                own[g][h, :half, part] = top
                own[g][h, half:, part] = low
                tsum[g][h, :half, part] = top.astype(BF16)
                tsum[g][h, half:, part] = low.astype(BF16)
        for h in range(2):
            p, plus, minus, far = axes[h][1]
            if f"U{g}" in plan:
                for d, dev in enumerate((plus, minus)):
                    land = pl.ds(d * eighth, eighth)
                    send(gsem(g, 4), tsum[g].at[h, sub8(p, 2, d)], qsum[g].at[h, 0, land], dev)
                    send(gsem(g, 0), tsum[g].at[h, sub8(p, 1 + 2 * d, 1 - d)], qsum[g].at[h, 1, land], dev)
                continue
            for i, (off, dev) in enumerate(((2, far), (1, plus), (3, minus))):
                send(gsem(g, 0), tsum[g].at[h, sub(p, off)], qsum[g].at[h, i], dev)

    def merge2(g):
        arrived(gsem(g, 4), qsum[g].at[:, 0])
        for h in range(2):
            p, plus, minus, _ = axes[h][1]
            for d, dev in enumerate((plus, minus)):
                land = pl.ds(d * eighth, eighth)
                mine = own[g][h, sub8(p, 1 + 2 * d, d)]
                tmrg[g][h, d] = (mine + qsum[g][h, 0, land].astype(F32)).astype(BF16)
                send(gsem(g, 0), tmrg[g].at[h, d], qsum[g].at[h, 2, land], dev)

    def gather(g):
        merged = f"U{g}" in plan
        arrived(gsem(g, 0), qsum[g].at[:, 1:] if merged else qsum[g])
        for h in range(2):
            p, plus, minus, far = axes[h][1]
            pf = axes[h][0][0]
            if merged:
                for d in range(2):
                    total = own[g][h, sub8(p, 0, d)]
                    total += qsum[g][h, 2, d * eighth : (d + 1) * eighth].astype(F32)
                    total += qsum[g][h, 1, (1 - d) * eighth : (2 - d) * eighth].astype(F32)
                    y[sub8(p, 0, d), cols(h, g, pf)] = total.astype(BF16)
            else:
                total = own[g][h, sub(p, 0)]
                total += qsum[g][h, 0].astype(F32) + qsum[g][h, 1].astype(F32) + qsum[g][h, 2].astype(F32)
                y[sub(p, 0), cols(h, g, pf)] = total.astype(BF16)
            mine = y.at[sub(p, 0), cols(h, g, pf)]
            for dev in (plus, minus) if f"V{g}" in plan else (far, plus, minus):
                send(gsem(g, 1), mine, mine, dev)

    def relay1(g):
        arrived(gsem(g, 1), qsum[g].at[:, 1:])
        for h in range(2):
            p, plus, minus, _ = axes[h][1]
            for d, dev in enumerate((plus, minus)):
                piece = y.at[sub8(p, 3 - 2 * d, d), cols(h, g, axes[h][0][0])]
                send(gsem(g, 5), piece, piece, dev)

    def gather2(g, direct=False):
        if f"V{g}" in plan:
            arrived(gsem(g, 5), qsum[g].at[:, 0])
        else:
            arrived(gsem(g, 1), qsum[g])
        for h in range(2):
            pf, plus, minus, far = axes[h][0]
            mine = y.at[:, cols(h, g, pf)]
            if direct:
                send(gsem(g, 3), mine, mine, far)
            for dev in (plus, minus):
                send(gsem(g, 2), mine, mine, dev)

    def relay(g):
        arrived(gsem(g, 2), y.at[:, : 4 * gwidths[g]])
        for h in range(2):
            pf, plus, minus, _ = axes[h][0]
            for d, dev in enumerate((plus, minus)):
                seg = lax.rem(pf + 3 - 2 * d, side)
                piece = y.at[pl.ds(half * d, half), cols(h, g, seg)]
                send(gsem(g, 3), piece, piece, dev)

    def last(g, direct=False):
        if direct:
            arrived(gsem(g, 2), y.at[:, : 4 * gwidths[g]])
        arrived(gsem(g, 3), y.at[:, : 2 * gwidths[g]])

    pl.semaphore_wait(barrier, 6)

    stages = {
        "X": functools.partial(down, (2,)), "Y": functools.partial(down, (1, 3, 0)),
        "M": merge, "S": second, "U": merge2, "V": relay1, "G": gather, "A": gather2, "R": relay, "L": last,
        "D": functools.partial(gather2, direct=True), "E": functools.partial(last, direct=True),
    }
    for token in plan:
        stages[token[0]](int(token[1]))

    wait_rows = sum(sent) // nblock
    flat = gub.reshape(-1, nblock)
    pltpu.make_async_copy(flat.at[:wait_rows], flat.at[:wait_rows], ssem).wait()


def block(n, x, w_gate, w_up, w_down):
    rows, d = x.shape
    ff = w_gate.shape[1]
    side = 4
    assert n == side * side
    unit = d // (2 * side * sum(sum(group) for group in GROUPS))
    groups = tuple(tuple(w * unit for w in group) for group in GROUPS)
    widths = [w for group in groups for w in group]
    kchunk, nblock = min(KCHUNK, d), min(NBLOCK, ff)
    half = rows // 2
    vm = pltpu.VMEM
    dma = pltpu.SemaphoreType.DMA
    chunk_scratch = []
    for w in map(sum, groups):
        chunk_scratch += [
            vm((2, rows, w), F32),
            vm((2, rows, w), BF16),
            vm((2, 3, rows // 4, w), BF16),
            vm((2, 2, rows // 8, w), BF16),
        ]
    for w in widths:
        chunk_scratch += [
            vm((2, 2, half, w), F32),
            vm((2, rows, w), BF16),
            vm((2, 2, half, w), BF16),
            vm((2, 2, half, w), BF16),
            vm((2, 2, half, w), BF16),
            vm((2, 4, half, w), BF16),
        ]
    hbm = pl.BlockSpec(memory_space=pltpu.HBM)
    return pl.pallas_call(
        functools.partial(kernel, groups, kchunk, nblock),
        out_shape=jax.ShapeDtypeStruct((rows, d), BF16),
        in_specs=[hbm] * 4,
        out_specs=pl.BlockSpec(memory_space=pltpu.VMEM),
        scratch_shapes=[
            vm((d // kchunk, rows, kchunk), BF16),
            vm((DEPTH, 2, kchunk, nblock), BF16),
            vm((AHEAD + 1, ff, 2 * max(widths)), BF16),
            vm((rows, nblock), F32),
            vm((rows, nblock), F32),
            vm((rows, ff), BF16),
            dma((d // kchunk,)),
            dma((DEPTH,)),
            dma((AHEAD + 1,)),
            dma(()),
            dma((2 * len(widths) + 6 * len(groups),)),
            *chunk_scratch,
        ],
        compiler_params=pltpu.CompilerParams(
            collective_id=0, has_side_effects=True, vmem_limit_bytes=50 * 2**20
        ),
        name="mlp",
    )(x, w_gate, w_up, w_down)


def solution(mesh):
    return jax.shard_map(
        functools.partial(block, mesh.shape["tp"]),
        mesh=mesh,
        in_specs=(P("dp", None), P(None, "tp"), P(None, "tp"), P("tp", None)),
        out_specs=P("dp", None),
        check_vma=False,
    )
```

```python
import functools

import jax
import jax.numpy as jnp
from jax import lax
from jax.experimental import pallas as pl
from jax.experimental.pallas import tpu as pltpu
from jax.sharding import PartitionSpec as P

MESH = pl.DeviceIdType.MESH
BF16, F32 = jnp.bfloat16, jnp.float32
GROUPS = ((2,), (2,), (2,), (2,))
NBLOCK = 512
KCHUNK = 1024
DEPTH = 4
AHEAD = 5
SCHEDULE = ('X0', 'X1', 'X2', 'X3', 'Y0', 'M0', 'Y1', 'M1', 'Y2', 'M2', 'Y3', 'M3', 'S0', 'S1', 'S2', 'S3', 'G0', 'G1', 'G2', 'G3', 'A0', 'A1', 'D2', 'D3', 'R0', 'R1', 'L0', 'L1', 'E2', 'E3')


def kernel(
    groups, kchunk, nblock,
    x_hbm, wg_hbm, wu_hbm, wd_hbm, y,
    xv, gub, wdb, accg, accu, hid,
    xsem, gusem, wsem, ssem, rsem, *chunk_refs,
):
    widths = [w for group in groups for w in group]
    split = 4 * len(groups)
    own, tsum, qsum, tmrg = (chunk_refs[i:split:4] for i in range(4))
    keep, sstep, sdir, smrg, rstep, rboth = (chunk_refs[split + i :: 6] for i in range(6))
    where = [(g, sum(group[:i])) for g, group in enumerate(groups) for i in range(len(group))]
    gwidths = [sum(group) for group in groups]

    side = 4
    me = lax.axis_index("tp")
    px, py = me // side, lax.rem(me, side)

    def at(i, j):
        return lax.rem(i + side, side) * side + lax.rem(j + side, side)

    along = (
        (px, at(px + 1, py), at(px - 1, py), at(px + 2, py)),
        (py, at(px, py + 1), at(px, py - 1), at(px, py + 2)),
    )
    axes = (along, along[::-1])

    rows = xv.shape[1]
    ksteps = wg_hbm.shape[0] // kchunk
    nblocks = wg_hbm.shape[1] // nblock
    steps = ksteps * nblocks
    half, quarter, eighth = rows // 2, rows // 4, rows // 8
    ring = wdb.shape[0]

    def xcopy(k):
        return pltpu.make_async_copy(x_hbm.at[:, pl.ds(k * kchunk, kchunk)], xv.at[k], xsem.at[k])

    def gstart(i, slot):
        nb, k = i // ksteps, lax.rem(i, ksteps)
        src = (pl.ds(k * kchunk, kchunk), pl.ds(nb * nblock, nblock))
        pltpu.make_async_copy(wg_hbm.at[src], gub.at[slot, 0], gusem.at[slot]).start()
        pltpu.make_async_copy(wu_hbm.at[src], gub.at[slot, 1], gusem.at[slot]).start()

    def gwait(slot):
        pltpu.make_async_copy(gub.at[slot], gub.at[slot], gusem.at[slot]).wait()

    def cols(h, g, seg, skip=0, width=None):
        first = h * sum(widths) * side + sum(gwidths[:g]) * side + skip
        return pl.ds(pl.multiple_of(first + seg * gwidths[g], 128), width or gwidths[g])

    plan = SCHEDULE
    order = []
    for token in plan:
        order += [(int(token[1]), off) for off in {"X": (2,), "Y": (1, 3, 0)}.get(token[0], ())]

    def wstart(j):
        c, off = order[j]
        g, skip = where[c]
        for h in range(2):
            seg = lax.rem(axes[h][0][0] + off, side)
            pltpu.make_async_copy(
                wd_hbm.at[:, cols(h, g, seg, skip, widths[c])],
                wdb.at[j % ring, :, h * widths[c] : (h + 1) * widths[c]],
                wsem.at[j % ring],
            ).start()

    def wwait(j):
        buf = wdb.at[j % ring, :, : 2 * widths[order[j][0]]]
        pltpu.make_async_copy(buf, buf, wsem.at[j % ring]).wait()

    for i in range(DEPTH):
        xcopy(i).start()
        gstart(jnp.int32(i), i)
    for k in range(DEPTH, ksteps):
        xcopy(k).start()

    barrier = pltpu.get_barrier_semaphore()
    for _, *partners in along:
        for dev in partners:
            pl.semaphore_signal(barrier, inc=1, device_id={"tp": dev}, device_id_type=MESH)

    for nb in range(nblocks):
        accg[...] = jnp.zeros_like(accg)
        accu[...] = jnp.zeros_like(accu)

        @pl.loop(0, ksteps)
        def _(k, nb=nb):
            i = nb * ksteps + k
            slot = lax.rem(i, DEPTH)
            if nb == 0:
                xcopy(k).wait()
            gwait(slot)
            accg[...] += jnp.dot(xv[k], gub[slot, 0], preferred_element_type=F32)
            accu[...] += jnp.dot(xv[k], gub[slot, 1], preferred_element_type=F32)

            @pl.when(i + DEPTH < steps)
            def _():
                gstart(i + DEPTH, slot)

            if nb == nblocks - 1:
                for d in range(DEPTH):

                    @pl.when(i + DEPTH == steps + d)
                    def _(d=d):
                        for j in range(d * AHEAD // DEPTH, (d + 1) * AHEAD // DEPTH):
                            wstart(j)

        g = accg[...]
        hid[:, nb * nblock : (nb + 1) * nblock] = (jax.nn.silu(g) * accu[...]).astype(BF16)

    sent = []

    def send(sem, src, dst, dev):
        pltpu.make_async_remote_copy(
            src_ref=src, dst_ref=dst, send_sem=ssem, recv_sem=rsem.at[sem],
            device_id={"tp": dev}, device_id_type=MESH,
        ).start()
        sent.append(src.shape[0] * src.shape[1])

    def arrived(sem, like):
        pltpu.make_async_copy(like, like, rsem.at[sem]).wait()

    def gsem(g, stage):
        return 2 * len(widths) + 6 * g + stage

    def down(offs, c):
        for off in offs:
            j = order.index((c, off))
            if j + AHEAD < len(order):
                wstart(j + AHEAD)
            wwait(j)
            width = widths[c]
            g, skip = where[c]
            both = jnp.dot(hid[...], wdb[j % ring, :, : 2 * width], preferred_element_type=F32)
            for h in range(2):
                _, plus, minus, _ = axes[h][0]
                t = both[:, h * width : (h + 1) * width]
                if off == 2:
                    sstep[c][h] = t.astype(BF16)
                    send(2 * c, sstep[c].at[h, :half], rstep[c].at[h, 0], plus)
                    send(2 * c, sstep[c].at[h, half:], rstep[c].at[h, 1], minus)
                elif off == 1:
                    keep[c][h, 0] = t[:half]
                    sdir[c][h, 0] = t[half:].astype(BF16)
                    send(2 * c + 1, sdir[c].at[h, 0], rboth[c].at[h, 2], plus)
                elif off == 3:
                    keep[c][h, 1] = t[half:]
                    sdir[c][h, 1] = t[:half].astype(BF16)
                    send(2 * c + 1, sdir[c].at[h, 1], rboth[c].at[h, 3], minus)
                else:
                    own[g][h, :, skip : skip + width] = t

    def merge(c):
        arrived(2 * c, rstep[c])
        for h in range(2):
            _, plus, minus, _ = axes[h][0]
            for d, dev in enumerate((plus, minus)):
                smrg[c][h, d] = (keep[c][h, d] + rstep[c][h, d].astype(F32)).astype(BF16)
                send(2 * c + 1, smrg[c].at[h, d], rboth[c].at[h, d], dev)

    def sub(p, off):
        return pl.ds(pl.multiple_of(lax.rem(p + off, side) * quarter, quarter), quarter)

    def sub8(p, off, low):
        return pl.ds(pl.multiple_of(lax.rem(p + off, side) * quarter + low * eighth, eighth), eighth)

    def second(g):
        for c, (at_g, skip) in enumerate(where):
            if at_g != g:
                continue
            arrived(2 * c + 1, rboth[c])
            part = slice(skip, skip + widths[c])
            for h in range(2):
                top = own[g][h, :half, part] + (rboth[c][h, 0].astype(F32) + rboth[c][h, 3].astype(F32))
                low = own[g][h, half:, part] + (rboth[c][h, 1].astype(F32) + rboth[c][h, 2].astype(F32))
                own[g][h, :half, part] = top
                own[g][h, half:, part] = low
                tsum[g][h, :half, part] = top.astype(BF16)
                tsum[g][h, half:, part] = low.astype(BF16)
        for h in range(2):
            p, plus, minus, far = axes[h][1]
            if f"U{g}" in plan:
                for d, dev in enumerate((plus, minus)):
                    land = pl.ds(d * eighth, eighth)
                    send(gsem(g, 4), tsum[g].at[h, sub8(p, 2, d)], qsum[g].at[h, 0, land], dev)
                    send(gsem(g, 0), tsum[g].at[h, sub8(p, 1 + 2 * d, 1 - d)], qsum[g].at[h, 1, land], dev)
                continue
            for i, (off, dev) in enumerate(((2, far), (1, plus), (3, minus))):
                send(gsem(g, 0), tsum[g].at[h, sub(p, off)], qsum[g].at[h, i], dev)

    def merge2(g):
        arrived(gsem(g, 4), qsum[g].at[:, 0])
        for h in range(2):
            p, plus, minus, _ = axes[h][1]
            for d, dev in enumerate((plus, minus)):
                land = pl.ds(d * eighth, eighth)
                mine = own[g][h, sub8(p, 1 + 2 * d, d)]
                tmrg[g][h, d] = (mine + qsum[g][h, 0, land].astype(F32)).astype(BF16)
                send(gsem(g, 0), tmrg[g].at[h, d], qsum[g].at[h, 2, land], dev)

    def gather(g):
        merged = f"U{g}" in plan
        arrived(gsem(g, 0), qsum[g].at[:, 1:] if merged else qsum[g])
        for h in range(2):
            p, plus, minus, far = axes[h][1]
            pf = axes[h][0][0]
            if merged:
                for d in range(2):
                    total = own[g][h, sub8(p, 0, d)]
                    total += qsum[g][h, 2, d * eighth : (d + 1) * eighth].astype(F32)
                    total += qsum[g][h, 1, (1 - d) * eighth : (2 - d) * eighth].astype(F32)
                    y[sub8(p, 0, d), cols(h, g, pf)] = total.astype(BF16)
            else:
                total = own[g][h, sub(p, 0)]
                total += qsum[g][h, 0].astype(F32) + qsum[g][h, 1].astype(F32) + qsum[g][h, 2].astype(F32)
                y[sub(p, 0), cols(h, g, pf)] = total.astype(BF16)
            mine = y.at[sub(p, 0), cols(h, g, pf)]
            for dev in (plus, minus) if f"V{g}" in plan else (far, plus, minus):
                send(gsem(g, 1), mine, mine, dev)
        for h in range(2):
            along_first(h, g, ((0, 0), (1, 0)))

    def along_first(h, g, pieces):
        p = axes[h][1][0]
        pf, plus, minus, far = axes[h][0]
        for d, off in pieces:
            piece = y.at[sub(p, off), cols(h, g, pf)]
            if f"D{g}" in plan:
                send(gsem(g, 2), piece, piece, (plus, minus)[d])
                if d == 0:
                    send(gsem(g, 3), piece, piece, far)
            else:
                relayed = (off < 2) == (d == 0)
                send(gsem(g, 2 if relayed else 3), piece, piece, (plus, minus)[d])

    def relay1(g):
        arrived(gsem(g, 1), qsum[g].at[:, 1:])
        for h in range(2):
            p, plus, minus, _ = axes[h][1]
            for d, dev in enumerate((plus, minus)):
                piece = y.at[sub8(p, 3 - 2 * d, d), cols(h, g, axes[h][0][0])]
                send(gsem(g, 5), piece, piece, dev)

    def gather2(g):
        if f"V{g}" in plan:
            arrived(gsem(g, 5), qsum[g].at[:, 0])
        else:
            arrived(gsem(g, 1), qsum[g])
        for h in range(2):
            along_first(h, g, ((0, 1), (1, 2), (1, 3), (1, 1), (0, 2), (0, 3)))

    def relay(g):
        arrived(gsem(g, 2), y.at[:, : 2 * gwidths[g]])
        for h in range(2):
            p = axes[h][1][0]
            pf, plus, minus, _ = axes[h][0]
            for d, dev in enumerate((plus, minus)):
                seg = lax.rem(pf + 3 - 2 * d, side)
                for off in (2 * d, 2 * d + 1):
                    piece = y.at[sub(p, off), cols(h, g, seg)]
                    send(gsem(g, 3), piece, piece, dev)

    def last(g, direct=False):
        if direct:
            arrived(gsem(g, 2), y.at[:, : 4 * gwidths[g]])
        arrived(gsem(g, 3), y.at[:, : (2 if direct else 4) * gwidths[g]])

    pl.semaphore_wait(barrier, 6)

    stages = {
        "X": functools.partial(down, (2,)), "Y": functools.partial(down, (1, 3, 0)),
        "M": merge, "S": second, "U": merge2, "V": relay1, "G": gather, "A": gather2, "R": relay, "L": last,
        "D": gather2, "E": functools.partial(last, direct=True),
    }
    for token in plan:
        stages[token[0]](int(token[1]))

    wait_rows = sum(sent) // nblock
    flat = gub.reshape(-1, nblock)
    pltpu.make_async_copy(flat.at[:wait_rows], flat.at[:wait_rows], ssem).wait()


def block(n, x, w_gate, w_up, w_down):
    rows, d = x.shape
    ff = w_gate.shape[1]
    side = 4
    assert n == side * side
    unit = d // (2 * side * sum(sum(group) for group in GROUPS))
    groups = tuple(tuple(w * unit for w in group) for group in GROUPS)
    widths = [w for group in groups for w in group]
    kchunk, nblock = min(KCHUNK, d), min(NBLOCK, ff)
    half = rows // 2
    vm = pltpu.VMEM
    dma = pltpu.SemaphoreType.DMA
    chunk_scratch = []
    for w in map(sum, groups):
        chunk_scratch += [
            vm((2, rows, w), F32),
            vm((2, rows, w), BF16),
            vm((2, 3, rows // 4, w), BF16),
            vm((2, 2, rows // 8, w), BF16),
        ]
    for w in widths:
        chunk_scratch += [
            vm((2, 2, half, w), F32),
            vm((2, rows, w), BF16),
            vm((2, 2, half, w), BF16),
            vm((2, 2, half, w), BF16),
            vm((2, 2, half, w), BF16),
            vm((2, 4, half, w), BF16),
        ]
    hbm = pl.BlockSpec(memory_space=pltpu.HBM)
    return pl.pallas_call(
        functools.partial(kernel, groups, kchunk, nblock),
        out_shape=jax.ShapeDtypeStruct((rows, d), BF16),
        in_specs=[hbm] * 4,
        out_specs=pl.BlockSpec(memory_space=pltpu.VMEM),
        scratch_shapes=[
            vm((d // kchunk, rows, kchunk), BF16),
            vm((DEPTH, 2, kchunk, nblock), BF16),
            vm((AHEAD + 1, ff, 2 * max(widths)), BF16),
            vm((rows, nblock), F32),
            vm((rows, nblock), F32),
            vm((rows, ff), BF16),
            dma((d // kchunk,)),
            dma((DEPTH,)),
            dma((AHEAD + 1,)),
            dma(()),
            dma((2 * len(widths) + 6 * len(groups),)),
            *chunk_scratch,
        ],
        compiler_params=pltpu.CompilerParams(
            collective_id=0, has_side_effects=True, vmem_limit_bytes=50 * 2**20
        ),
        name="mlp",
    )(x, w_gate, w_up, w_down)


def solution(mesh):
    return jax.shard_map(
        functools.partial(block, mesh.shape["tp"]),
        mesh=mesh,
        in_specs=(P("dp", None), P(None, "tp"), P(None, "tp"), P("tp", None)),
        out_specs=P("dp", None),
        check_vma=False,
    )
```

```python
import functools

import jax
import jax.numpy as jnp
from jax import lax
from jax.experimental import pallas as pl
from jax.experimental.pallas import tpu as pltpu
from jax.sharding import PartitionSpec as P

MESH = pl.DeviceIdType.MESH
BF16, F32 = jnp.bfloat16, jnp.float32
GROUPS = ((2,), (2,), (2,), (2,))
NBLOCK = 768
KCHUNK = 1024
DEPTH = 4
AHEAD = 5
SCHEDULE = ('X0', 'X1', 'X2', 'X3', 'Y0', 'M0', 'Y1', 'M1', 'Y2', 'M2', 'Y3', 'M3', 'S0', 'S1', 'S2', 'S3', 'G0', 'G1', 'G2', 'G3', 'A0', 'A1', 'D2', 'D3', 'R0', 'R1')


def kernel(
    groups, kchunk, nblock,
    x_hbm, wg_hbm, wu_hbm, wd_hbm, y,
    xv, gub, wdb, accg, accu, hid,
    xsem, gusem, wsem, ssem, rsem, *chunk_refs,
):
    widths = [w for group in groups for w in group]
    split = 3 * len(groups)
    own, tsum, qsum = (chunk_refs[i:split:3] for i in range(3))
    keep, sstep, sdir, smrg, rstep, rboth = (chunk_refs[split + i :: 6] for i in range(6))
    where = [(g, sum(group[:i])) for g, group in enumerate(groups) for i in range(len(group))]
    gwidths = [sum(group) for group in groups]

    side = 4
    me = lax.axis_index("tp")
    px, py = me // side, lax.rem(me, side)

    def at(i, j):
        return lax.rem(i + side, side) * side + lax.rem(j + side, side)

    along = (
        (px, at(px + 1, py), at(px - 1, py), at(px + 2, py)),
        (py, at(px, py + 1), at(px, py - 1), at(px, py + 2)),
    )
    axes = (along, along[::-1])

    rows = xv.shape[1]
    ksteps = wg_hbm.shape[0] // kchunk
    nblocks = wg_hbm.shape[1] // nblock
    steps = ksteps * nblocks
    half, quarter = rows // 2, rows // 4
    ring = wdb.shape[0]

    def xcopy(k):
        return pltpu.make_async_copy(x_hbm.at[:, pl.ds(k * kchunk, kchunk)], xv.at[k], xsem.at[k])

    def gstart(i, slot):
        nb, k = i // ksteps, lax.rem(i, ksteps)
        src = (pl.ds(k * kchunk, kchunk), pl.ds(nb * nblock, nblock))
        pltpu.make_async_copy(wg_hbm.at[src], gub.at[slot, 0], gusem.at[slot]).start()
        pltpu.make_async_copy(wu_hbm.at[src], gub.at[slot, 1], gusem.at[slot]).start()

    def gwait(slot):
        pltpu.make_async_copy(gub.at[slot], gub.at[slot], gusem.at[slot]).wait()

    def cols(h, g, seg, skip=0, width=None):
        first = h * sum(widths) * side + sum(gwidths[:g]) * side + skip
        return pl.ds(pl.multiple_of(first + seg * gwidths[g], 128), width or gwidths[g])

    plan = SCHEDULE
    order = []
    for token in plan:
        order += [(int(token[1]), off) for off in {"X": (2,), "Y": (1, 3, 0)}.get(token[0], ())]

    def wstart(j):
        c, off = order[j]
        g, skip = where[c]
        for h in range(2):
            seg = lax.rem(axes[h][0][0] + off, side)
            pltpu.make_async_copy(
                wd_hbm.at[:, cols(h, g, seg, skip, widths[c])],
                wdb.at[j % ring, :, h * widths[c] : (h + 1) * widths[c]],
                wsem.at[j % ring],
            ).start()

    def wwait(j):
        buf = wdb.at[j % ring, :, : 2 * widths[order[j][0]]]
        pltpu.make_async_copy(buf, buf, wsem.at[j % ring]).wait()

    for i in range(DEPTH):
        xcopy(i).start()
        gstart(jnp.int32(i), i)
    for k in range(DEPTH, ksteps):
        xcopy(k).start()

    barrier = pltpu.get_barrier_semaphore()
    for _, *partners in along:
        for dev in partners:
            pl.semaphore_signal(barrier, inc=1, device_id={"tp": dev}, device_id_type=MESH)

    for nb in range(nblocks):
        accg[...] = jnp.zeros_like(accg)
        accu[...] = jnp.zeros_like(accu)

        @pl.loop(0, ksteps)
        def _(k, nb=nb):
            i = nb * ksteps + k
            slot = lax.rem(i, DEPTH)
            if nb == 0:
                xcopy(k).wait()
            gwait(slot)
            accg[...] += jnp.dot(xv[k], gub[slot, 0], preferred_element_type=F32)
            accu[...] += jnp.dot(xv[k], gub[slot, 1], preferred_element_type=F32)

            @pl.when(i + DEPTH < steps)
            def _():
                gstart(i + DEPTH, slot)

            if nb == nblocks - 1:
                for d in range(DEPTH):

                    @pl.when(i + DEPTH == steps + d)
                    def _(d=d):
                        for j in range(d * AHEAD // DEPTH, (d + 1) * AHEAD // DEPTH):
                            wstart(j)

        g = accg[...]
        hid[:, nb * nblock : (nb + 1) * nblock] = (jax.nn.silu(g) * accu[...]).astype(BF16)

    sent = []

    def send(sem, src, dst, dev):
        pltpu.make_async_remote_copy(
            src_ref=src, dst_ref=dst, send_sem=ssem, recv_sem=rsem.at[sem],
            device_id={"tp": dev}, device_id_type=MESH,
        ).start()
        sent.append(src.shape[0] * src.shape[1])

    def arrived(sem, like):
        pltpu.make_async_copy(like, like, rsem.at[sem]).wait()

    def gsem(g, stage):
        return 2 * len(widths) + (0 if stage == 3 else 1 + 3 * g + stage)

    def down(offs, c):
        for off in offs:
            j = order.index((c, off))
            if j + AHEAD < len(order):
                wstart(j + AHEAD)
            wwait(j)
            width = widths[c]
            g, skip = where[c]
            both = jnp.dot(hid[...], wdb[j % ring, :, : 2 * width], preferred_element_type=F32)
            for h in range(2):
                _, plus, minus, _ = axes[h][0]
                t = both[:, h * width : (h + 1) * width]
                if off == 2:
                    sstep[c][h] = t.astype(BF16)
                    send(2 * c, sstep[c].at[h, :half], rstep[c].at[h, 0], plus)
                    send(2 * c, sstep[c].at[h, half:], rstep[c].at[h, 1], minus)
                elif off == 1:
                    keep[c][h, 0] = t[:half]
                    sdir[c][h, 0] = t[half:].astype(BF16)
                    send(2 * c + 1, sdir[c].at[h, 0], rboth[c].at[h, 2], plus)
                elif off == 3:
                    keep[c][h, 1] = t[half:]
                    sdir[c][h, 1] = t[:half].astype(BF16)
                    send(2 * c + 1, sdir[c].at[h, 1], rboth[c].at[h, 3], minus)
                else:
                    own[g][h, :, skip : skip + width] = t

    def merge(c):
        arrived(2 * c, rstep[c])
        for h in range(2):
            _, plus, minus, _ = axes[h][0]
            for d, dev in enumerate((plus, minus)):
                smrg[c][h, d] = (keep[c][h, d] + rstep[c][h, d].astype(F32)).astype(BF16)
                send(2 * c + 1, smrg[c].at[h, d], rboth[c].at[h, d], dev)

    def sub(p, off):
        return pl.ds(pl.multiple_of(lax.rem(p + off, side) * quarter, quarter), quarter)

    def second(g):
        for c, (at_g, skip) in enumerate(where):
            if at_g != g:
                continue
            arrived(2 * c + 1, rboth[c])
            part = slice(skip, skip + widths[c])
            for h in range(2):
                top = own[g][h, :half, part] + (rboth[c][h, 0].astype(F32) + rboth[c][h, 3].astype(F32))
                low = own[g][h, half:, part] + (rboth[c][h, 1].astype(F32) + rboth[c][h, 2].astype(F32))
                own[g][h, :half, part] = top
                own[g][h, half:, part] = low
                tsum[g][h, :half, part] = top.astype(BF16)
                tsum[g][h, half:, part] = low.astype(BF16)
        for h in range(2):
            p, plus, minus, far = axes[h][1]
            for i, (off, dev) in enumerate(((2, far), (1, plus), (3, minus))):
                send(gsem(g, 0), tsum[g].at[h, sub(p, off)], qsum[g].at[h, i], dev)

    def gather(g):
        arrived(gsem(g, 0), qsum[g])
        for h in range(2):
            p, plus, minus, far = axes[h][1]
            pf = axes[h][0][0]
            total = own[g][h, sub(p, 0)]
            total += qsum[g][h, 0].astype(F32) + qsum[g][h, 1].astype(F32) + qsum[g][h, 2].astype(F32)
            y[sub(p, 0), cols(h, g, pf)] = total.astype(BF16)
            mine = y.at[sub(p, 0), cols(h, g, pf)]
            for dev in (far, plus, minus):
                send(gsem(g, 1), mine, mine, dev)
        for h in range(2):
            along_first(h, g, ((0, 0), (1, 0)))

    def along_first(h, g, pieces):
        p = axes[h][1][0]
        pf, plus, minus, far = axes[h][0]
        for d, off in pieces:
            piece = y.at[sub(p, off), cols(h, g, pf)]
            if f"D{g}" in plan:
                send(gsem(g, 2), piece, piece, (plus, minus)[d])
                if d == 0:
                    send(gsem(g, 3), piece, piece, far)
            else:
                relayed = (off < 2) == (d == 0)
                send(gsem(g, 2 if relayed else 3), piece, piece, (plus, minus)[d])

    def gather2(g):
        arrived(gsem(g, 1), qsum[g])
        for h in range(2):
            along_first(h, g, ((0, 1), (1, 2), (1, 3), (1, 1), (0, 2), (0, 3)))

    def relay(g):
        arrived(gsem(g, 2), y.at[:, : 2 * gwidths[g]])
        for h in range(2):
            p = axes[h][1][0]
            pf, plus, minus, _ = axes[h][0]
            for d, dev in enumerate((plus, minus)):
                seg = lax.rem(pf + 3 - 2 * d, side)
                for off in (2 * d, 2 * d + 1):
                    piece = y.at[sub(p, off), cols(h, g, seg)]
                    send(gsem(g, 3), piece, piece, dev)

    pl.semaphore_wait(barrier, 6)

    stages = {
        "X": functools.partial(down, (2,)), "Y": functools.partial(down, (1, 3, 0)),
        "M": merge, "S": second, "G": gather, "A": gather2, "R": relay, "D": gather2,
    }
    for token in plan:
        stages[token[0]](int(token[1]))

    total = 0
    for g, w in enumerate(gwidths):
        if f"D{g}" in plan:
            arrived(gsem(g, 2), y.at[:, : 4 * w])
        total += (2 if f"D{g}" in plan else 4) * w
    arrived(gsem(0, 3), y.at[:, :total])

    wait_rows = sum(sent) // nblock
    assert wait_rows * nblock == sum(sent)
    flat = gub.reshape(-1, nblock)
    pltpu.make_async_copy(flat.at[:wait_rows], flat.at[:wait_rows], ssem).wait()


def block(n, x, w_gate, w_up, w_down):
    rows, d = x.shape
    ff = w_gate.shape[1]
    side = 4
    assert n == side * side
    unit = d // (2 * side * sum(sum(group) for group in GROUPS))
    groups = tuple(tuple(w * unit for w in group) for group in GROUPS)
    widths = [w for group in groups for w in group]
    kchunk, nblock = min(KCHUNK, d), min(NBLOCK, ff)
    half = rows // 2
    vm = pltpu.VMEM
    dma = pltpu.SemaphoreType.DMA
    chunk_scratch = []
    for w in map(sum, groups):
        chunk_scratch += [
            vm((2, rows, w), F32),
            vm((2, rows, w), BF16),
            vm((2, 3, rows // 4, w), BF16),
        ]
    for w in widths:
        chunk_scratch += [
            vm((2, 2, half, w), F32),
            vm((2, rows, w), BF16),
            vm((2, 2, half, w), BF16),
            vm((2, 2, half, w), BF16),
            vm((2, 2, half, w), BF16),
            vm((2, 4, half, w), BF16),
        ]
    hbm = pl.BlockSpec(memory_space=pltpu.HBM)
    return pl.pallas_call(
        functools.partial(kernel, groups, kchunk, nblock),
        out_shape=jax.ShapeDtypeStruct((rows, d), BF16),
        in_specs=[hbm] * 4,
        out_specs=pl.BlockSpec(memory_space=pltpu.VMEM),
        scratch_shapes=[
            vm((d // kchunk, rows, kchunk), BF16),
            vm((DEPTH, 2, kchunk, nblock), BF16),
            vm((AHEAD + 1, ff, 2 * max(widths)), BF16),
            vm((rows, nblock), F32),
            vm((rows, nblock), F32),
            vm((rows, ff), BF16),
            dma((d // kchunk,)),
            dma((DEPTH,)),
            dma((AHEAD + 1,)),
            dma(()),
            dma((2 * len(widths) + 1 + 3 * len(groups),)),
            *chunk_scratch,
        ],
        compiler_params=pltpu.CompilerParams(
            collective_id=0, has_side_effects=True, vmem_limit_bytes=50 * 2**20
        ),
        name="mlp",
    )(x, w_gate, w_up, w_down)


def solution(mesh):
    return jax.shard_map(
        functools.partial(block, mesh.shape["tp"]),
        mesh=mesh,
        in_specs=(P("dp", None), P(None, "tp"), P(None, "tp"), P("tp", None)),
        out_specs=P("dp", None),
        check_vma=False,
    )
```

```python
import functools

import jax
import jax.numpy as jnp
from jax import lax
from jax.experimental import pallas as pl
from jax.experimental.pallas import tpu as pltpu
from jax.sharding import PartitionSpec as P

MESH = pl.DeviceIdType.MESH
BF16, F32 = jnp.bfloat16, jnp.float32
GROUPS = ((2,), (2,), (2,), (1,), (1,))
NBLOCK = 768
KCHUNK = 1024
DEPTH = 4
AHEAD = 5
SCHEDULE = ('X0', 'X1', 'X2', 'X3', 'X4', 'Y0', 'M0', 'Y1', 'M1', 'Y2', 'M2', 'Y3', 'M3', 'Y4', 'M4', 'S0', 'S1', 'S2', 'S3', 'S4', 'G0', 'G1', 'G2', 'G3', 'G4', 'A0', 'A1', 'A2', 'D3', 'D4', 'R0', 'R1', 'R2')


def kernel(
    groups, kchunk, nblock,
    x_hbm, wg_hbm, wu_hbm, wd_hbm, y,
    xv, gub, wdb, accg, accu, hid,
    xsem, gusem, wsem, ssem, rsem, *chunk_refs,
):
    widths = [w for group in groups for w in group]
    split = 3 * len(groups)
    own, tsum, qsum = (chunk_refs[i:split:3] for i in range(3))
    keep, sstep, sdir, smrg, rstep, rboth = (chunk_refs[split + i :: 6] for i in range(6))
    where = [(g, sum(group[:i])) for g, group in enumerate(groups) for i in range(len(group))]
    gwidths = [sum(group) for group in groups]

    side = 4
    me = lax.axis_index("tp")
    px, py = me // side, lax.rem(me, side)

    def at(i, j):
        return lax.rem(i + side, side) * side + lax.rem(j + side, side)

    along = (
        (px, at(px + 1, py), at(px - 1, py), at(px + 2, py)),
        (py, at(px, py + 1), at(px, py - 1), at(px, py + 2)),
    )
    axes = (along, along[::-1])

    rows = xv.shape[1]
    ksteps = wg_hbm.shape[0] // kchunk
    nblocks = wg_hbm.shape[1] // nblock
    steps = ksteps * nblocks
    half, quarter = rows // 2, rows // 4
    ring = wdb.shape[0]

    def xcopy(k):
        return pltpu.make_async_copy(x_hbm.at[:, pl.ds(k * kchunk, kchunk)], xv.at[k], xsem.at[k])

    def gstart(i, slot):
        nb, k = i // ksteps, lax.rem(i, ksteps)
        src = (pl.ds(k * kchunk, kchunk), pl.ds(nb * nblock, nblock))
        pltpu.make_async_copy(wg_hbm.at[src], gub.at[slot, 0], gusem.at[slot]).start()
        pltpu.make_async_copy(wu_hbm.at[src], gub.at[slot, 1], gusem.at[slot]).start()

    def gwait(slot):
        pltpu.make_async_copy(gub.at[slot], gub.at[slot], gusem.at[slot]).wait()

    def cols(h, g, seg, skip=0, width=None):
        first = h * sum(widths) * side + sum(gwidths[:g]) * side + skip
        return pl.ds(pl.multiple_of(first + seg * gwidths[g], 128), width or gwidths[g])

    plan = SCHEDULE
    order = []
    for token in plan:
        order += [(int(token[1]), off) for off in {"X": (2,), "Y": (1, 3, 0)}.get(token[0], ())]

    def wstart(j):
        c, off = order[j]
        g, skip = where[c]
        for h in range(2):
            seg = lax.rem(axes[h][0][0] + off, side)
            pltpu.make_async_copy(
                wd_hbm.at[:, cols(h, g, seg, skip, widths[c])],
                wdb.at[j % ring, :, h * widths[c] : (h + 1) * widths[c]],
                wsem.at[j % ring],
            ).start()

    def wwait(j):
        buf = wdb.at[j % ring, :, : 2 * widths[order[j][0]]]
        pltpu.make_async_copy(buf, buf, wsem.at[j % ring]).wait()

    for i in range(DEPTH):
        xcopy(i).start()
        gstart(jnp.int32(i), i)
    for k in range(DEPTH, ksteps):
        xcopy(k).start()

    barrier = pltpu.get_barrier_semaphore()
    for _, *partners in along:
        for dev in partners:
            pl.semaphore_signal(barrier, inc=1, device_id={"tp": dev}, device_id_type=MESH)

    for nb in range(nblocks):
        accg[...] = jnp.zeros_like(accg)
        accu[...] = jnp.zeros_like(accu)

        @pl.loop(0, ksteps)
        def _(k, nb=nb):
            i = nb * ksteps + k
            slot = lax.rem(i, DEPTH)
            if nb == 0:
                xcopy(k).wait()
            gwait(slot)
            accg[...] += jnp.dot(xv[k], gub[slot, 0], preferred_element_type=F32)
            accu[...] += jnp.dot(xv[k], gub[slot, 1], preferred_element_type=F32)

            @pl.when(i + DEPTH < steps)
            def _():
                gstart(i + DEPTH, slot)

            if nb == nblocks - 1:
                for d in range(DEPTH):

                    @pl.when(i + DEPTH == steps + d)
                    def _(d=d):
                        for j in range(d * AHEAD // DEPTH, (d + 1) * AHEAD // DEPTH):
                            wstart(j)

        g = accg[...]
        hid[:, nb * nblock : (nb + 1) * nblock] = (jax.nn.silu(g) * accu[...]).astype(BF16)

    sent = []

    def send(sem, src, dst, dev):
        pltpu.make_async_remote_copy(
            src_ref=src, dst_ref=dst, send_sem=ssem, recv_sem=rsem.at[sem],
            device_id={"tp": dev}, device_id_type=MESH,
        ).start()
        sent.append(src.shape[0] * src.shape[1])

    def arrived(sem, like):
        pltpu.make_async_copy(like, like, rsem.at[sem]).wait()

    def gsem(g, stage):
        return 2 * len(widths) + (0 if stage == 3 else 1 + 3 * g + stage)

    def down(offs, c):
        for off in offs:
            j = order.index((c, off))
            if j + AHEAD < len(order):
                wstart(j + AHEAD)
            wwait(j)
            width = widths[c]
            g, skip = where[c]
            both = jnp.dot(hid[...], wdb[j % ring, :, : 2 * width], preferred_element_type=F32)
            for h in range(2):
                _, plus, minus, _ = axes[h][0]
                t = both[:, h * width : (h + 1) * width]
                if off == 2:
                    sstep[c][h] = t.astype(BF16)
                    send(2 * c, sstep[c].at[h, :half], rstep[c].at[h, 0], plus)
                    send(2 * c, sstep[c].at[h, half:], rstep[c].at[h, 1], minus)
                elif off == 1:
                    keep[c][h, 0] = t[:half]
                    sdir[c][h, 0] = t[half:].astype(BF16)
                    send(2 * c + 1, sdir[c].at[h, 0], rboth[c].at[h, 2], plus)
                elif off == 3:
                    keep[c][h, 1] = t[half:]
                    sdir[c][h, 1] = t[:half].astype(BF16)
                    send(2 * c + 1, sdir[c].at[h, 1], rboth[c].at[h, 3], minus)
                else:
                    own[g][h, :, skip : skip + width] = t

    def merge(c):
        arrived(2 * c, rstep[c])
        for h in range(2):
            _, plus, minus, _ = axes[h][0]
            for d, dev in enumerate((plus, minus)):
                smrg[c][h, d] = (keep[c][h, d] + rstep[c][h, d].astype(F32)).astype(BF16)
                send(2 * c + 1, smrg[c].at[h, d], rboth[c].at[h, d], dev)

    def sub(p, off):
        return pl.ds(pl.multiple_of(lax.rem(p + off, side) * quarter, quarter), quarter)

    def second(g):
        for c, (at_g, skip) in enumerate(where):
            if at_g != g:
                continue
            arrived(2 * c + 1, rboth[c])
            part = slice(skip, skip + widths[c])
            for h in range(2):
                top = own[g][h, :half, part] + (rboth[c][h, 0].astype(F32) + rboth[c][h, 3].astype(F32))
                low = own[g][h, half:, part] + (rboth[c][h, 1].astype(F32) + rboth[c][h, 2].astype(F32))
                own[g][h, :half, part] = top
                own[g][h, half:, part] = low
                tsum[g][h, :half, part] = top.astype(BF16)
                tsum[g][h, half:, part] = low.astype(BF16)
        for h in range(2):
            p, plus, minus, far = axes[h][1]
            for i, (off, dev) in enumerate(((2, far), (1, plus), (3, minus))):
                send(gsem(g, 0), tsum[g].at[h, sub(p, off)], qsum[g].at[h, i], dev)

    def gather(g):
        arrived(gsem(g, 0), qsum[g])
        for h in range(2):
            p, plus, minus, far = axes[h][1]
            pf = axes[h][0][0]
            total = own[g][h, sub(p, 0)]
            total += qsum[g][h, 0].astype(F32) + qsum[g][h, 1].astype(F32) + qsum[g][h, 2].astype(F32)
            y[sub(p, 0), cols(h, g, pf)] = total.astype(BF16)
            mine = y.at[sub(p, 0), cols(h, g, pf)]
            for dev in (far, plus, minus):
                send(gsem(g, 1), mine, mine, dev)
        for h in range(2):
            along_first(h, g, ((0, 0), (1, 0)))

    def along_first(h, g, pieces):
        p = axes[h][1][0]
        pf, plus, minus, far = axes[h][0]
        for d, off in pieces:
            piece = y.at[sub(p, off), cols(h, g, pf)]
            if f"D{g}" in plan:
                send(gsem(g, 2), piece, piece, (plus, minus)[d])
                if d == 0:
                    send(gsem(g, 3), piece, piece, far)
            else:
                relayed = (off < 2) == (d == 0)
                send(gsem(g, 2 if relayed else 3), piece, piece, (plus, minus)[d])

    def gather2(g):
        arrived(gsem(g, 1), qsum[g])
        for h in range(2):
            along_first(h, g, ((0, 1), (1, 2), (1, 3), (1, 1), (0, 2), (0, 3)))

    def relay(g):
        arrived(gsem(g, 2), y.at[:, : 2 * gwidths[g]])
        for h in range(2):
            p = axes[h][1][0]
            pf, plus, minus, _ = axes[h][0]
            for d, dev in enumerate((plus, minus)):
                seg = lax.rem(pf + 3 - 2 * d, side)
                for off in (2 * d, 2 * d + 1):
                    piece = y.at[sub(p, off), cols(h, g, seg)]
                    send(gsem(g, 3), piece, piece, dev)

    pl.semaphore_wait(barrier, 6)

    stages = {
        "X": functools.partial(down, (2,)), "Y": functools.partial(down, (1, 3, 0)),
        "M": merge, "S": second, "G": gather, "A": gather2, "R": relay, "D": gather2,
    }
    for token in plan:
        stages[token[0]](int(token[1]))

    total = 0
    for g, w in enumerate(gwidths):
        if f"D{g}" in plan:
            arrived(gsem(g, 2), y.at[:, : 4 * w])
        total += (2 if f"D{g}" in plan else 4) * w
    arrived(gsem(0, 3), y.at[:, :total])

    wait_rows = sum(sent) // nblock
    assert wait_rows * nblock == sum(sent)
    flat = gub.reshape(-1, nblock)
    pltpu.make_async_copy(flat.at[:wait_rows], flat.at[:wait_rows], ssem).wait()


def block(n, x, w_gate, w_up, w_down):
    rows, d = x.shape
    ff = w_gate.shape[1]
    side = 4
    assert n == side * side
    unit = d // (2 * side * sum(sum(group) for group in GROUPS))
    groups = tuple(tuple(w * unit for w in group) for group in GROUPS)
    widths = [w for group in groups for w in group]
    kchunk, nblock = min(KCHUNK, d), min(NBLOCK, ff)
    half = rows // 2
    vm = pltpu.VMEM
    dma = pltpu.SemaphoreType.DMA
    chunk_scratch = []
    for w in map(sum, groups):
        chunk_scratch += [
            vm((2, rows, w), F32),
            vm((2, rows, w), BF16),
            vm((2, 3, rows // 4, w), BF16),
        ]
    for w in widths:
        chunk_scratch += [
            vm((2, 2, half, w), F32),
            vm((2, rows, w), BF16),
            vm((2, 2, half, w), BF16),
            vm((2, 2, half, w), BF16),
            vm((2, 2, half, w), BF16),
            vm((2, 4, half, w), BF16),
        ]
    hbm = pl.BlockSpec(memory_space=pltpu.HBM)
    return pl.pallas_call(
        functools.partial(kernel, groups, kchunk, nblock),
        out_shape=jax.ShapeDtypeStruct((rows, d), BF16),
        in_specs=[hbm] * 4,
        out_specs=pl.BlockSpec(memory_space=pltpu.VMEM),
        scratch_shapes=[
            vm((d // kchunk, rows, kchunk), BF16),
            vm((DEPTH, 2, kchunk, nblock), BF16),
            vm((AHEAD + 1, ff, 2 * max(widths)), BF16),
            vm((rows, nblock), F32),
            vm((rows, nblock), F32),
            vm((rows, ff), BF16),
            dma((d // kchunk,)),
            dma((DEPTH,)),
            dma((AHEAD + 1,)),
            dma(()),
            dma((2 * len(widths) + 1 + 3 * len(groups),)),
            *chunk_scratch,
        ],
        compiler_params=pltpu.CompilerParams(
            collective_id=0, has_side_effects=True, vmem_limit_bytes=50 * 2**20
        ),
        name="mlp",
    )(x, w_gate, w_up, w_down)


def solution(mesh):
    return jax.shard_map(
        functools.partial(block, mesh.shape["tp"]),
        mesh=mesh,
        in_specs=(P("dp", None), P(None, "tp"), P(None, "tp"), P("tp", None)),
        out_specs=P("dp", None),
        check_vma=False,
    )
```
